32 devices in a mesh: bank: 8 (over z, y), ens: 4 (over x, core).
Axes of the slice: x: 2, y: 2, z: 4, core: 2. Of those that a mesh axis runs over, the one named last changes fastest.
Arguments:
- item_ids: int32 [1024, 2], P(('ens', 'bank')), parts along dimension 0, may hold values from 0 to 2047
- large_table: bfloat16 [8192, 256], P(('ens', 'bank')), parts along dimension 0, may hold values from -6 to 6
- dense_part: float32 [1024, 256], P(('ens', 'bank')), parts along dimension 0, may hold values from -6 to 6
- small_ids: int32 [1024], P(('ens', 'bank')), parts along dimension 0, may hold values from 0 to 15
- small_table: bfloat16 [64, 256], P(('ens', 'bank')), parts along dimension 0, may hold values from -6 to 6
- scale_ids: int32 [1024], P(('ens', 'bank')), parts along dimension 0, may hold values from 0 to 15
Outputs:
- features: float32 [1024, 256], P(('ens', 'bank')), parts along dimension 0
The draws below stay inside these ranges and needn't reach their ends.
There are 4 independent parts, one for each index of `ens`. The reference program is written for one: setup_inputs(seed, part) draws one part's arguments, and reference() takes and returns one part's arrays. A program takes and returns all parts, laid end to end along the dimension named above; each array names one. Nothing has to cross between parts.
All inputs are finite; a program needn't handle non-finite values.
Results may differ from the reference program's by a relative error of at most 0.0003.
Values may be sent and summed in bfloat16 or wider, within the bound.
A program may use at most 64 MiB of HBM per device.

```python
import math
import jax
import jax.numpy as jnp
import numpy as np
from jax import lax

EXAMPLES = 256
FEATURES = 256
PICKS = 2
BIG_ROWS = 2048
SMALL_ROWS = 16


def place_ends(result, own_key, least, high):
    dims = result.shape
    index_at = [jax.random.randint(jax.random.fold_in(own_key, axis), (), 0, dims[axis]) for axis in range(len(dims))]
    result = result.at[tuple(index_at)].set(least)
    longest = dims.index(max(dims))
    index_at[longest] = (index_at[longest] + 1) % dims[longest]
    return result.at[tuple(index_at)].set(high)


def steps_of(own_key, dims, cuts, smallest, largest):
    level = 1.0
    for dim, shards_of in cuts:
        steps = jax.random.uniform(jax.random.fold_in(jax.random.fold_in(own_key, 6), dim), (shards_of,), jnp.float32, smallest / len(cuts), largest / len(cuts))
        level = level * jnp.repeat(jnp.exp(steps), dims[dim] // shards_of).reshape((-1,) + (1,) * (len(dims) - 1 - dim))
    return level


def rank_table(number_of, skew):
    loads = [(1 << 20) // math.isqrt(grade ** skew) + 1 for grade in range(1, number_of + 1)]
    scale = 1 + sum(loads) // (1 << 30)
    return np.cumsum(np.array([max(1, weight // scale) for weight in loads]))


def ranked_ids(own_key, extent, number_of, skew):
    grid = rank_table(number_of, skew)
    ticket = jax.random.randint(jax.random.fold_in(own_key, 1), extent, 0, int(grid[number_of - 1]))
    standing = jnp.searchsorted(jnp.asarray(grid, jnp.int32), ticket, side="right")
    return jax.random.permutation(jax.random.fold_in(own_key, 2), number_of)[standing].astype(jnp.int32)


def gaussian(stream_key, dims, spread, bound, cuts=(), kind=jnp.bfloat16):
    factor_of = steps_of(stream_key, dims, cuts, -0.22, 0.18) if cuts else 1.0
    values = jax.random.normal(stream_key, dims, jnp.float32) * spread * factor_of
    return jnp.minimum(jnp.maximum(values, -bound), bound).astype(kind)


def setup_inputs(seed: int = 0, part: int = 0) -> dict:
    seeds = jax.random.split(jax.random.key(seed), 7)
    part_keys = jax.random.split(jax.random.fold_in(seeds[6], part), 7)
    item_ids = place_ends(ranked_ids(part_keys[0], (EXAMPLES, PICKS), BIG_ROWS, 1), jax.random.fold_in(part_keys[0], 3), 0, BIG_ROWS - 1).astype(jnp.int32)
    large_table = gaussian(part_keys[1], (BIG_ROWS, FEATURES), 1.0, 6.0, ((0, 8),))
    dense_part = gaussian(part_keys[2], (EXAMPLES, FEATURES), 1.0, 6.0, ((0, 8),), jnp.float32)
    small_ids = place_ends(jax.random.randint(part_keys[3], (EXAMPLES,), 0, SMALL_ROWS), jax.random.fold_in(part_keys[3], 1), 0, SMALL_ROWS - 1).astype(jnp.int32)
    small_table = gaussian(part_keys[4], (SMALL_ROWS, FEATURES), 1.0, 6.0, ((0, 8),))
    scale_ids = place_ends(ranked_ids(part_keys[5], (EXAMPLES,), SMALL_ROWS, 1), jax.random.fold_in(part_keys[5], 3), 0, SMALL_ROWS - 1).astype(jnp.int32)
    return {"item_ids": item_ids, "large_table": large_table, "dense_part": dense_part, "small_ids": small_ids, "small_table": small_table, "scale_ids": scale_ids}


def reference(item_ids, large_table, dense_part, small_ids, small_table, scale_ids):
    pooled = lax.optimization_barrier(jnp.sum(large_table[item_ids].astype(jnp.float32), axis=1)) * PICKS ** (-0.5)
    small_rows = small_table[small_ids].astype(jnp.float32)
    dense_part = dense_part * small_table[scale_ids].astype(jnp.float32)
    total = dense_part + pooled * small_rows
    features = total * lax.rsqrt(lax.optimization_barrier(jnp.mean(total * total, axis=-1, keepdims=True)) + 1e-06)
    return features
```

```python
import functools

import jax
import jax.numpy as jnp
from jax import lax
from jax.experimental import pallas as pl
from jax.experimental.pallas import tpu as pltpu
from jax.sharding import PartitionSpec as P

MESH = pl.DeviceIdType.MESH
PICKS = 2
CHUNKS = 2


def column(row, eye):
    wide = jnp.where(eye, row.astype(jnp.float32), 0.0)
    return jnp.sum(wide, axis=1, keepdims=True)


def kernel(n, ids_in, tab_in, dense_in, sid_in, small_in, cid_in, out, ids, tab, dense, sid, small, cid, part, got,
           lsem, tsem, ids_s, ids_r, tab_s, tab_r, sp_s, sp_r, sl_s, sl_r, part_s, part_r):
    line = n // 2
    me = lax.axis_index("bank")
    z, y = lax.div(me, 2), lax.rem(me, 2)
    partner = me + 1 - 2 * y
    rows, feats = tab_in.shape
    examples = dense_in.shape[0]
    width = feats // CHUNKS

    def on_line(d):
        return lax.rem(z + line + d, line) * 2 + y

    def cols(c):
        return pl.ds(c * width, width)

    local = [
        pltpu.make_async_copy(ids_in, ids.at[0], lsem.at[0]),
        pltpu.make_async_copy(small_in, small.at[z, y], lsem.at[1]),
        pltpu.make_async_copy(sid_in, sid, lsem.at[2]),
        pltpu.make_async_copy(cid_in, cid, lsem.at[3]),
        pltpu.make_async_copy(dense_in, dense, lsem.at[4]),
    ]
    tables = [
        pltpu.make_async_copy(tab_in.at[:, cols(c)], tab.at[0, c], tsem.at[c]) for c in range(CHUNKS)
    ]
    for copy in local[:2] + tables + local[2:]:
        copy.start()

    barrier = pltpu.get_barrier_semaphore()
    for other in [on_line(d) for d in range(1, line)] + [partner]:
        pl.semaphore_signal(barrier, inc=1, device_id={"bank": other}, device_id_type=MESH)
    pl.semaphore_wait(barrier, line)

    def remote(src, dst, send, recv, other):
        return pltpu.make_async_remote_copy(
            src_ref=src, dst_ref=dst, send_sem=send, recv_sem=recv, device_id={"bank": other}, device_id_type=MESH
        )

    sends = []
    local[0].wait()
    id_copies = [remote(ids.at[0], ids.at[d], ids_s.at[d], ids_r.at[d], on_line(d)) for d in range(1, line)]
    for copy in id_copies:
        copy.start()
    tab_copies = []
    for c in range(CHUNKS):
        tables[c].wait()
        copy = remote(tab.at[0, c], tab.at[1, c], tab_s.at[c], tab_r.at[c], partner)
        copy.start()
        tab_copies.append(copy)
        if c == 0:
            local[1].wait()
            small_pair = remote(small.at[z, y], small.at[z, y], sp_s.at[0], sp_r.at[0], partner)
            small_pair.start()
    for copy in local[2:]:
        copy.wait()

    eye = lax.broadcasted_iota(jnp.int32, (examples, examples), 0) == lax.broadcasted_iota(
        jnp.int32, (examples, examples), 1
    )
    lanes = lax.broadcasted_iota(jnp.int32, (1, rows), 1).astype(jnp.float32)
    first = [(owner * rows).astype(jnp.float32) for owner in (me, partner)]

    for copy in id_copies:
        copy.wait_recv()
    counts = [[], []]
    for d in range(line):
        picks = [column(ids[d, p : p + 1, :], eye) for p in range(PICKS)]
        for side in range(2):
            at = lanes + first[side]
            counts[side].append(sum(jnp.where(pick == at, 1.0, 0.0) for pick in picks))
    counts = [jnp.concatenate(c, axis=0).astype(jnp.bfloat16) for c in counts]

    part_copies = []
    kept = []
    for c in range(CHUNKS):
        mine = jnp.dot(counts[0], tab[0, c], preferred_element_type=jnp.float32)
        tab_copies[c].wait_recv()
        both = mine + jnp.dot(counts[1], tab[1, c], preferred_element_type=jnp.float32)
        part[c] = both
        for d in range(1, line):
            copy = remote(
                part.at[c, pl.ds(d * examples, examples)], got.at[c, d], part_s.at[c, d], part_r.at[c, d], on_line(-d)
            )
            copy.start()
            part_copies.append(copy)
        if c == 0:
            small_pair.wait_recv()
            small_line = [remote(small.at[z], small.at[z], sl_s.at[d], sl_r.at[d], on_line(d)) for d in range(1, line)]
            for copy in small_line:
                copy.start()

    for copy in small_line:
        copy.wait_recv()
    small_id, scale_id = column(sid[...], eye), column(cid[...], eye)
    small_rows = jnp.zeros((examples, feats), jnp.float32)
    scale_rows = jnp.zeros((examples, feats), jnp.float32)
    held = small_in.shape[0]
    for b in range(n):
        block = small[b // 2, b % 2].astype(jnp.float32)
        for r in range(held):
            row = block[r : r + 1, :]
            small_rows = jnp.where(small_id == float(b * held + r), row, small_rows)
            scale_rows = jnp.where(scale_id == float(b * held + r), row, scale_rows)
    base = dense[...] * scale_rows

    totals = []
    for c in range(CHUNKS):
        pooled = part[c, :examples]
        for d in range(1, line):
            part_copies[c * (line - 1) + d - 1].wait_recv()
            pooled = pooled + got[c, d]
        span = slice(c * width, (c + 1) * width)
        totals.append(base[:, span] + pooled * PICKS ** (-0.5) * small_rows[:, span])
    power = sum(jnp.sum(t * t, axis=1, keepdims=True) for t in totals) * (1.0 / feats)
    scale = lax.rsqrt(power + 1e-06)
    for c in range(CHUNKS):
        out[:, cols(c)] = totals[c] * scale
    for copy in id_copies + tab_copies + [small_pair] + small_line + part_copies:
        copy.wait_send()


def solution(mesh):
    n = mesh.shape["bank"]
    line = n // 2

    def shards(item_ids, large_table, dense_part, small_ids, small_table, scale_ids):
        rows, feats = large_table.shape
        examples = dense_part.shape[0]
        held = small_table.shape[0]
        width = feats // CHUNKS
        dma = pltpu.SemaphoreType.DMA
        return pl.pallas_call(
            functools.partial(kernel, n),
            out_shape=jax.ShapeDtypeStruct((examples, feats), jnp.float32),
            in_specs=[pl.BlockSpec(memory_space=pl.ANY)] * 6,
            out_specs=pl.BlockSpec(memory_space=pltpu.VMEM),
            scratch_shapes=[
                pltpu.VMEM((line, PICKS, examples), jnp.int32),
                pltpu.VMEM((2, CHUNKS, rows, width), jnp.bfloat16),
                pltpu.VMEM((examples, feats), jnp.float32),
                pltpu.VMEM((1, examples), jnp.int32),
                pltpu.VMEM((line, 2, held, feats), jnp.bfloat16),
                pltpu.VMEM((1, examples), jnp.int32),
                pltpu.VMEM((CHUNKS, line * examples, width), jnp.float32),
                pltpu.VMEM((CHUNKS, line, examples, width), jnp.float32),
                dma((5,)),
                dma((CHUNKS,)),
                dma((line,)),
                dma((line,)),
                dma((CHUNKS,)),
                dma((CHUNKS,)),
                dma((1,)),
                dma((1,)),
                dma((line,)),
                dma((line,)),
                dma((CHUNKS, line)),
                dma((CHUNKS, line)),
            ],
            compiler_params=pltpu.CompilerParams(collective_id=0, has_side_effects=True),
        )(
            item_ids.T,
            large_table,
            dense_part,
            small_ids.reshape(1, -1),
            small_table,
            scale_ids.reshape(1, -1),
        )

    return jax.shard_map(
        shards,
        mesh=mesh,
        in_specs=(
            P(("ens", "bank"), None),
            P(("ens", "bank"), None),
            P(("ens", "bank"), None),
            P(("ens", "bank")),
            P(("ens", "bank"), None),
            P(("ens", "bank")),
        ),
        out_specs=P(("ens", "bank"), None),
        check_vma=False,
    )
```

```python
import functools

import jax
import jax.numpy as jnp
from jax import lax
from jax.experimental import pallas as pl
from jax.experimental.pallas import tpu as pltpu
from jax.sharding import PartitionSpec as P

MESH = pl.DeviceIdType.MESH
PICKS = 2
CHUNKS = 2


def column(row, eye):
    wide = jnp.where(eye, row.astype(jnp.float32), 0.0)
    return jnp.sum(wide, axis=1, keepdims=True)


def kernel(n, ids_in, tab_in, dense_in, sid_in, small_in, cid_in, out, ids, tab, dense, sid, small, cid, part, got,
           lsem, tsem, ids_s, ids_r, tab_s, tab_r, sp_s, sp_r, sl_s, sl_r, part_s, part_r):
    line = n // 2
    me = lax.axis_index("bank")
    z, y = lax.div(me, 2), lax.rem(me, 2)
    partner = me + 1 - 2 * y
    rows, feats = tab_in.shape
    examples = dense_in.shape[0]
    width = feats // CHUNKS

    sign = 1 - 2 * lax.div(2 * z, line)

    def spot(d):
        return lax.rem(z + line + sign * d, line)

    def on_line(d):
        return spot(d) * 2 + y

    away = range(line - 1, 0, -1)

    def cols(c):
        return pl.ds(c * width, width)

    local = [
        pltpu.make_async_copy(ids_in, ids.at[z], lsem.at[0]),
        pltpu.make_async_copy(small_in, small.at[z, y], lsem.at[1]),
        pltpu.make_async_copy(sid_in, sid, lsem.at[2]),
        pltpu.make_async_copy(cid_in, cid, lsem.at[3]),
        pltpu.make_async_copy(dense_in, dense, lsem.at[4]),
    ]
    tables = [
        pltpu.make_async_copy(tab_in.at[:, cols(c)], tab.at[0, c], tsem.at[c]) for c in range(CHUNKS)
    ]
    for copy in local[:2] + tables + local[2:]:
        copy.start()

    barrier = pltpu.get_barrier_semaphore()
    for other in [on_line(d) for d in away] + [partner]:
        pl.semaphore_signal(barrier, inc=1, device_id={"bank": other}, device_id_type=MESH)
    pl.semaphore_wait(barrier, line)

    def remote(src, dst, send, recv, other):
        return pltpu.make_async_remote_copy(
            src_ref=src, dst_ref=dst, send_sem=send, recv_sem=recv, device_id={"bank": other}, device_id_type=MESH
        )

    def landed(ref, recv):
        remote(ref, ref, ids_s.at[0], recv, partner).wait_recv()

    local[0].wait()
    id_copies = [remote(ids.at[z], ids.at[z], ids_s.at[d], ids_r.at[z], on_line(d)) for d in away]
    for copy in id_copies:
        copy.start()
    tab_copies = []
    for c in range(CHUNKS):
        tables[c].wait()
        copy = remote(tab.at[0, c], tab.at[1, c], tab_s.at[c], tab_r.at[c], partner)
        copy.start()
        tab_copies.append(copy)
        if c == 0:
            local[1].wait()
            small_pair = remote(small.at[z, y], small.at[z, y], sp_s.at[0], sp_r.at[0], partner)
            small_pair.start()
    for copy in local[2:]:
        copy.wait()

    eye = lax.broadcasted_iota(jnp.int32, (examples, examples), 0) == lax.broadcasted_iota(
        jnp.int32, (examples, examples), 1
    )
    lanes = lax.broadcasted_iota(jnp.int32, (1, rows), 1).astype(jnp.float32)
    first = [(owner * rows).astype(jnp.float32) for owner in (me, partner)]

    for d in away:
        landed(ids.at[spot(d)], ids_r.at[spot(d)])
    counts = [[], []]
    for d in range(line):
        picks = [column(ids[d, p : p + 1, :], eye) for p in range(PICKS)]
        for side in range(2):
            at = lanes + first[side]
            counts[side].append(sum(jnp.where(pick == at, 1.0, 0.0) for pick in picks))
    counts = [jnp.concatenate(c, axis=0).astype(jnp.bfloat16) for c in counts]

    part_copies = []
    kept = []
    for c in range(CHUNKS):
        mine = jnp.dot(counts[0], tab[0, c], preferred_element_type=jnp.float32)
        tab_copies[c].wait_recv()
        both = mine + jnp.dot(counts[1], tab[1, c], preferred_element_type=jnp.float32)
        part[c] = both
        for d in away:
            share = pl.ds(pl.multiple_of(spot(d) * examples, examples), examples)
            copy = remote(part.at[c, share], got.at[c, z], part_s.at[c, d], part_r.at[c, z], on_line(d))
            copy.start()
            part_copies.append(copy)
        if c == 0:
            small_pair.wait_recv()
            small_line = [remote(small.at[z], small.at[z], sl_s.at[d], sl_r.at[z], on_line(d)) for d in away]
            for copy in small_line:
                copy.start()

    for d in away:
        landed(small.at[spot(d)], sl_r.at[spot(d)])
    small_id, scale_id = column(sid[...], eye), column(cid[...], eye)
    small_rows = jnp.zeros((examples, feats), jnp.float32)
    scale_rows = jnp.zeros((examples, feats), jnp.float32)
    held = small_in.shape[0]
    for b in range(n):
        block = small[b // 2, b % 2].astype(jnp.float32)
        for r in range(held):
            row = block[r : r + 1, :]
            small_rows = jnp.where(small_id == float(b * held + r), row, small_rows)
            scale_rows = jnp.where(scale_id == float(b * held + r), row, scale_rows)
    base = dense[...] * scale_rows

    totals = []
    for c in range(CHUNKS):
        pooled = part[c, pl.ds(pl.multiple_of(z * examples, examples), examples)]
        for d in range(1, line):
            landed(got.at[c, spot(d)], part_r.at[c, spot(d)])
            pooled = pooled + got[c, spot(d)]
        span = slice(c * width, (c + 1) * width)
        totals.append(base[:, span] + pooled * PICKS ** (-0.5) * small_rows[:, span])
    power = sum(jnp.sum(t * t, axis=1, keepdims=True) for t in totals) * (1.0 / feats)
    scale = lax.rsqrt(power + 1e-06)
    for c in range(CHUNKS):
        out[:, cols(c)] = totals[c] * scale
    for copy in id_copies + tab_copies + [small_pair] + small_line + part_copies:
        copy.wait_send()


def solution(mesh):
    n = mesh.shape["bank"]
    line = n // 2

    def shards(item_ids, large_table, dense_part, small_ids, small_table, scale_ids):
        rows, feats = large_table.shape
        examples = dense_part.shape[0]
        held = small_table.shape[0]
        width = feats // CHUNKS
        dma = pltpu.SemaphoreType.DMA
        return pl.pallas_call(
            functools.partial(kernel, n),
            out_shape=pltpu.VMEM((examples, feats), jnp.float32),
            in_specs=[pl.BlockSpec(memory_space=pltpu.HBM)] * 6,
            out_specs=pl.BlockSpec(memory_space=pltpu.VMEM),
            scratch_shapes=[
                pltpu.VMEM((line, PICKS, examples), jnp.int32),
                pltpu.VMEM((2, CHUNKS, rows, width), jnp.bfloat16),
                pltpu.VMEM((examples, feats), jnp.float32),
                pltpu.VMEM((1, examples), jnp.int32),
                pltpu.VMEM((line, 2, held, feats), jnp.bfloat16),
                pltpu.VMEM((1, examples), jnp.int32),
                pltpu.VMEM((CHUNKS, line * examples, width), jnp.float32),
                pltpu.VMEM((CHUNKS, line, examples, width), jnp.float32),
                dma((5,)),
                dma((CHUNKS,)),
                dma((line,)),
                dma((line,)),
                dma((CHUNKS,)),
                dma((CHUNKS,)),
                dma((1,)),
                dma((1,)),
                dma((line,)),
                dma((line,)),
                dma((CHUNKS, line)),
                dma((CHUNKS, line)),
            ],
            compiler_params=pltpu.CompilerParams(
                collective_id=0, has_side_effects=True
            ),
        )(
            item_ids.T,
            large_table,
            dense_part,
            small_ids.reshape(1, -1),
            small_table,
            scale_ids.reshape(1, -1),
        )

    return jax.shard_map(
        shards,
        mesh=mesh,
        in_specs=(
            P(("ens", "bank"), None),
            P(("ens", "bank"), None),
            P(("ens", "bank"), None),
            P(("ens", "bank")),
            P(("ens", "bank"), None),
            P(("ens", "bank")),
        ),
        out_specs=P(("ens", "bank"), None),
        check_vma=False,
    )
```

```python
import functools

import jax
import jax.numpy as jnp
from jax import lax
from jax.experimental import pallas as pl
from jax.experimental.pallas import tpu as pltpu
from jax.sharding import PartitionSpec as P

MESH = pl.DeviceIdType.MESH
PICKS = 2
CHUNKS = 2


def column(row, eye):
    wide = jnp.where(eye, row.astype(jnp.float32), 0.0)
    return jnp.sum(wide, axis=1, keepdims=True)


def kernel(n, ids_in, tab_in, dense_in, sid_in, small_in, cid_in, out, ids, tab, dense, sid, small, cid, part, got, raw,
           lsem, tsem, ids_s, ids_r, tab_s, tab_r, sp_s, sp_r, sl_s, sl_r, part_s, part_r, raw_s, raw_r, near, here):
    line = n // 2
    me = lax.axis_index("bank")
    z, y = lax.div(me, 2), lax.rem(me, 2)
    partner = me + 1 - 2 * y
    rows, feats = tab_in.shape
    examples = dense_in.shape[0]
    width = feats // CHUNKS

    sign = 1 - 2 * lax.div(2 * z, line)

    def spot(d):
        return lax.rem(z + line + sign * d, line)

    def on_line(d):
        return spot(d) * 2 + y

    away = range(line - 1, 0, -1)

    def cols(c):
        return pl.ds(c * width, width)

    local = [
        pltpu.make_async_copy(ids_in, ids.at[z], lsem.at[0]),
        pltpu.make_async_copy(small_in, small.at[z, y], lsem.at[1]),
        pltpu.make_async_copy(sid_in, sid, lsem.at[2]),
        pltpu.make_async_copy(cid_in, cid, lsem.at[3]),
        pltpu.make_async_copy(dense_in, dense, lsem.at[4]),
    ]
    tables = [
        pltpu.make_async_copy(tab_in.at[:, cols(c)], tab.at[0, c], tsem.at[c]) for c in range(CHUNKS)
    ]
    for copy in local[:2] + tables + local[2:]:
        copy.start()

    pusher = me >= n - 2
    head, tail, corner = me == 0, me == n - 2, me == n - 1

    def unless(condition, is_far, action):
        if is_far:
            pl.when(jnp.logical_not(condition))(action)
        else:
            action()

    barrier = pltpu.get_barrier_semaphore()

    def greet(other):
        pl.semaphore_signal(barrier, inc=1, device_id={"bank": other}, device_id_type=MESH)

    @pl.when(head)
    def _():
        greet(n - 1)

    for d in away:
        pl.when(spot(d) > z)(lambda d=d: greet(on_line(d)))
    pl.when(y == 0)(lambda: greet(partner))
    pl.when(me > 0)(lambda: pl.semaphore_wait(barrier, z + y + corner.astype(jnp.int32)))

    def answer(sem, other):
        pl.semaphore_signal(sem, inc=1, device_id={"bank": other}, device_id_type=MESH)

    for d in away:
        pl.when(spot(d) < z)(lambda d=d: answer(here.at[z], on_line(d)))
    pl.when(y == 1)(lambda: answer(near, partner))

    def hear(d):
        pl.when(spot(d) > z)(lambda: pl.semaphore_wait(here.at[spot(d)], 1))

    def remote(src, dst, send, recv, other):
        return pltpu.make_async_remote_copy(
            src_ref=src, dst_ref=dst, send_sem=send, recv_sem=recv, device_id={"bank": other}, device_id_type=MESH
        )

    def landed(ref, recv):
        remote(ref, ref, ids_s.at[0], recv, partner).wait_recv()

    local[0].wait()
    id_copies = {d: remote(ids.at[z], ids.at[z], ids_s.at[d], ids_r.at[z], on_line(d)) for d in away}
    for d in away:
        pl.when(spot(d) < z)(id_copies[d].start)
    for c in range(CHUNKS):
        tables[c].wait()
    raw_copies = [remote(tab.at[0, c], raw.at[y, c], raw_s.at[c], raw_r.at[y, c], 0) for c in range(CHUNKS)]
    tab_copies = [remote(tab.at[0, c], tab.at[1, c], tab_s.at[c], tab_r.at[c], partner) for c in range(CHUNKS)]
    local[1].wait()
    small_pair = remote(small.at[z, y], small.at[z, y], sp_s.at[0], sp_r.at[0], partner)

    def start_pair():
        for copy in [small_pair] + tab_copies:
            copy.start()

    pl.when(y == 1)(start_pair)

    @pl.when(pusher)
    def _():
        for copy in raw_copies:
            copy.start()

    def send_ids(d):
        hear(d)
        pl.when(spot(d) > z)(id_copies[d].start)

    if line > 1:
        unless(head, line == 2, lambda: send_ids(1))

    @pl.when(y == 0)
    def _():
        pl.semaphore_wait(near, 1)
        start_pair()

    for d in range(2, line):
        unless(head, d == line - 1, lambda d=d: send_ids(d))
    for copy in local[2:]:
        copy.wait()

    eye = lax.broadcasted_iota(jnp.int32, (examples, examples), 0) == lax.broadcasted_iota(
        jnp.int32, (examples, examples), 1
    )
    lanes = lax.broadcasted_iota(jnp.int32, (1, rows), 1).astype(jnp.float32)
    first = [(owner * rows).astype(jnp.float32) for owner in (me, partner)]

    def counted(spot_of):
        picks = [column(ids[spot_of, p : p + 1, :], eye) for p in range(PICKS)]
        return [sum(jnp.where(pick == lanes + f, 1.0, 0.0) for pick in picks).astype(jnp.bfloat16) for f in first]

    def summed(counts, c):
        return sum(jnp.dot(counts[side], tab[side, c], preferred_element_type=jnp.float32) for side in range(2))

    small_line = {d: remote(small.at[z], small.at[z], sl_s.at[d], sl_r.at[z], on_line(d)) for d in away}
    small_pair.wait_recv()
    for d in away:
        unless(head, d == line - 1, small_line[d].start)
    part_copies = []
    for d in range(1, line):
        unless(tail, d == line - 1, lambda d=d: landed(ids.at[spot(d)], ids_r.at[spot(d)]))
        if d == line - 1:

            @pl.when(head)
            def _():
                pl.semaphore_wait(here.at[spot(line - 1)], 1)

        counts = counted(spot(d))
        for c in range(CHUNKS):
            if d == 1:
                tab_copies[c].wait_recv()
            part[c, d] = summed(counts, c)
            copy = remote(part.at[c, d], got.at[c, z], part_s.at[c, d], part_r.at[c, z], on_line(d))
            unless(tail, d == line - 1, copy.start)
            part_copies.append((d, copy))
    pl.when(head)(small_line[line - 1].start)
    if line == 1:
        for copy in tab_copies:
            copy.wait_recv()
    counts = counted(z)
    kept = [summed(counts, c) for c in range(CHUNKS)]

    for d in away:
        landed(small.at[spot(d)], sl_r.at[spot(d)])
    small_id, scale_id = column(sid[...], eye), column(cid[...], eye)
    small_rows = jnp.zeros((examples, feats), jnp.float32)
    scale_rows = jnp.zeros((examples, feats), jnp.float32)
    held = small_in.shape[0]
    for b in range(n):
        block = small[b // 2, b % 2].astype(jnp.float32)
        for r in range(held):
            row = block[r : r + 1, :]
            small_rows = jnp.where(small_id == float(b * held + r), row, small_rows)
            scale_rows = jnp.where(scale_id == float(b * held + r), row, scale_rows)
    base = dense[...] * scale_rows

    @pl.when(head)
    def _():
        own_picks = [column(ids[z, p : p + 1, :], eye) for p in range(PICKS)]
        at = [lanes + float((n - 2 + side) * rows) for side in range(2)]
        for c in range(CHUNKS):
            far = jnp.zeros((examples, width), jnp.float32)
            for side in range(2):
                landed(raw.at[side, c], raw_r.at[side, c])
                count = sum(jnp.where(pick == at[side], 1.0, 0.0) for pick in own_picks).astype(jnp.bfloat16)
                far = far + jnp.dot(count, raw[side, c], preferred_element_type=jnp.float32)
            got[c, line - 1] = far

    totals = []
    for c in range(CHUNKS):
        pooled = kept[c]
        for d in range(1, line):
            unless(head, d == line - 1, lambda d=d: landed(got.at[c, spot(d)], part_r.at[c, spot(d)]))
            pooled = pooled + got[c, spot(d)]
        span = slice(c * width, (c + 1) * width)
        totals.append(base[:, span] + pooled * PICKS ** (-0.5) * small_rows[:, span])
    power = sum(jnp.sum(t * t, axis=1, keepdims=True) for t in totals) * (1.0 / feats)
    scale = lax.rsqrt(power + 1e-06)
    for c in range(CHUNKS):
        out[:, cols(c)] = totals[c] * scale
    for copy in tab_copies + [small_pair] + list(small_line.values()):
        copy.wait_send()
    for d, copy in id_copies.items():
        unless(head, d == line - 1, copy.wait_send)
    for d, copy in part_copies:
        unless(tail, d == line - 1, copy.wait_send)

    @pl.when(pusher)
    def _():
        for copy in raw_copies:
            copy.wait_send()


def solution(mesh):
    n = mesh.shape["bank"]
    line = n // 2

    def shards(item_ids, large_table, dense_part, small_ids, small_table, scale_ids):
        rows, feats = large_table.shape
        examples = dense_part.shape[0]
        held = small_table.shape[0]
        width = feats // CHUNKS
        dma = pltpu.SemaphoreType.DMA
        return pl.pallas_call(
            functools.partial(kernel, n),
            out_shape=pltpu.VMEM((examples, feats), jnp.float32),
            in_specs=[pl.BlockSpec(memory_space=pltpu.HBM)] * 6,
            out_specs=pl.BlockSpec(memory_space=pltpu.VMEM),
            scratch_shapes=[
                pltpu.VMEM((line, PICKS, examples), jnp.int32),
                pltpu.VMEM((2, CHUNKS, rows, width), jnp.bfloat16),
                pltpu.VMEM((examples, feats), jnp.float32),
                pltpu.VMEM((1, examples), jnp.int32),
                pltpu.VMEM((line, 2, held, feats), jnp.bfloat16),
                pltpu.VMEM((1, examples), jnp.int32),
                pltpu.VMEM((CHUNKS, line, examples, width), jnp.float32),
                pltpu.VMEM((CHUNKS, line, examples, width), jnp.float32),
                pltpu.VMEM((2, CHUNKS, rows, width), jnp.bfloat16),
                dma((5,)),
                dma((CHUNKS,)),
                dma((line,)),
                dma((line,)),
                dma((CHUNKS,)),
                dma((CHUNKS,)),
                dma((1,)),
                dma((1,)),
                dma((line,)),
                dma((line,)),
                dma((CHUNKS, line)),
                dma((CHUNKS, line)),
                dma((CHUNKS,)),
                dma((2, CHUNKS)),
                pltpu.SemaphoreType.REGULAR,
                pltpu.SemaphoreType.REGULAR((line,)),
            ],
            compiler_params=pltpu.CompilerParams(
                collective_id=0, has_side_effects=True
            ),
        )(
            item_ids.T,
            large_table,
            dense_part,
            small_ids.reshape(1, -1),
            small_table,
            scale_ids.reshape(1, -1),
        )

    return jax.shard_map(
        shards,
        mesh=mesh,
        in_specs=(
            P(("ens", "bank"), None),
            P(("ens", "bank"), None),
            P(("ens", "bank"), None),
            P(("ens", "bank")),
            P(("ens", "bank"), None),
            P(("ens", "bank")),
        ),
        out_specs=P(("ens", "bank"), None),
        check_vma=False,
    )
```

```python
import functools

import jax
import jax.numpy as jnp
from jax import lax
from jax.experimental import pallas as pl
from jax.experimental.pallas import tpu as pltpu
from jax.sharding import PartitionSpec as P

MESH = pl.DeviceIdType.MESH
PICKS = 2
CHUNKS = 2


def column(row, eye):
    wide = jnp.where(eye, row.astype(jnp.float32), 0.0)
    return jnp.sum(wide, axis=1, keepdims=True)


def kernel(n, ids_in, tab_in, dense_in, sid_in, small_in, cid_in, out, ids, tab, dense, sid, small, cid, part, got, raw,
           lsem, tsem, ids_s, ids_r, tab_s, tab_r, sp_s, sp_r, sl_s, sl_r, part_s, part_r, raw_s, raw_r, near, here):
    line = n // 2
    me = lax.axis_index("bank")
    z, y = lax.div(me, 2), lax.rem(me, 2)
    partner = me + 1 - 2 * y
    rows, feats = tab_in.shape
    examples = dense_in.shape[0]
    width = feats // CHUNKS

    sign = 1 - 2 * lax.div(2 * z, line)

    def spot(d):
        return lax.rem(z + line + sign * d, line)

    def on_line(d):
        return spot(d) * 2 + y

    away = range(line - 1, 0, -1)

    def cols(c):
        return pl.ds(c * width, width)

    local = [
        pltpu.make_async_copy(ids_in, ids.at[z], lsem.at[0]),
        pltpu.make_async_copy(small_in, small.at[z, y], lsem.at[1]),
        pltpu.make_async_copy(sid_in, sid, lsem.at[2]),
        pltpu.make_async_copy(cid_in, cid, lsem.at[3]),
        pltpu.make_async_copy(dense_in, dense, lsem.at[4]),
    ]
    tables = [
        pltpu.make_async_copy(tab_in.at[:, cols(c)], tab.at[0, c], tsem.at[c]) for c in range(CHUNKS)
    ]
    for copy in local[:2] + tables + local[2:]:
        copy.start()

    pusher = me >= n - 2
    head, tail, corner = me == 0, me == n - 2, me == n - 1

    def unless(condition, is_far, action):
        if is_far:
            pl.when(jnp.logical_not(condition))(action)
        else:
            action()

    barrier = pltpu.get_barrier_semaphore()

    def greet(other):
        pl.semaphore_signal(barrier, inc=1, device_id={"bank": other}, device_id_type=MESH)

    @pl.when(head)
    def _():
        greet(n - 1)

    for d in away:
        pl.when(spot(d) > z)(lambda d=d: greet(on_line(d)))
    pl.when(y == 0)(lambda: greet(partner))
    pl.when(me > 0)(lambda: pl.semaphore_wait(barrier, z + y + corner.astype(jnp.int32)))

    def answer(sem, other):
        pl.semaphore_signal(sem, inc=1, device_id={"bank": other}, device_id_type=MESH)

    for d in away:
        pl.when(spot(d) < z)(lambda d=d: answer(here.at[z], on_line(d)))
    pl.when(y == 1)(lambda: answer(near, partner))

    def hear(d):
        pl.when(spot(d) > z)(lambda: pl.semaphore_wait(here.at[spot(d)], 1))

    def remote(src, dst, send, recv, other):
        return pltpu.make_async_remote_copy(
            src_ref=src, dst_ref=dst, send_sem=send, recv_sem=recv, device_id={"bank": other}, device_id_type=MESH
        )

    def landed(ref, recv):
        remote(ref, ref, ids_s.at[0], recv, partner).wait_recv()

    local[0].wait()
    id_copies = {d: remote(ids.at[z], ids.at[z], ids_s.at[d], ids_r.at[z], on_line(d)) for d in away}
    for d in away:
        pl.when(spot(d) < z)(id_copies[d].start)
    for c in range(CHUNKS):
        tables[c].wait()
    raw_copies = [remote(tab.at[0, c], raw.at[y, c], raw_s.at[c], raw_r.at[y, c], 0) for c in range(CHUNKS)]
    tab_copies = [remote(tab.at[0, c], tab.at[1, c], tab_s.at[c], tab_r.at[c], partner) for c in range(CHUNKS)]
    local[1].wait()
    small_pair = remote(small.at[z, y], small.at[z, y], sp_s.at[0], sp_r.at[0], partner)

    def start_pair():
        for copy in [small_pair] + tab_copies:
            copy.start()

    pl.when(y == 1)(start_pair)

    @pl.when(pusher)
    def _():
        for copy in raw_copies:
            copy.start()

    def send_ids(d):
        hear(d)
        pl.when(spot(d) > z)(id_copies[d].start)

    if line > 1:
        unless(head, line == 2, lambda: send_ids(1))

    @pl.when(y == 0)
    def _():
        pl.semaphore_wait(near, 1)
        start_pair()

    for d in range(2, line):
        unless(head, d == line - 1, lambda d=d: send_ids(d))
    for copy in local[2:]:
        copy.wait()

    eye = lax.broadcasted_iota(jnp.int32, (examples, examples), 0) == lax.broadcasted_iota(
        jnp.int32, (examples, examples), 1
    )
    lanes = lax.broadcasted_iota(jnp.int32, (1, rows), 1).astype(jnp.float32)
    first = [(owner * rows).astype(jnp.float32) for owner in (me, partner)]

    def counted(spot_of):
        picks = [column(ids[spot_of, p : p + 1, :], eye) for p in range(PICKS)]
        return [sum(jnp.where(pick == lanes + f, 1.0, 0.0) for pick in picks).astype(jnp.bfloat16) for f in first]

    def summed(counts, c):
        return sum(jnp.dot(counts[side], tab[side, c], preferred_element_type=jnp.float32) for side in range(2))

    small_line = {d: remote(small.at[z], small.at[z], sl_s.at[d], sl_r.at[z], on_line(d)) for d in away}
    small_pair.wait_recv()
    for d in away:
        unless(head, d == line - 1, small_line[d].start)
    part_copies = []
    counts = {}
    for c in range(CHUNKS):
        tab_copies[c].wait_recv()
        for d in range(1, line):
            if c == 0:
                unless(tail, d == line - 1, lambda d=d: landed(ids.at[spot(d)], ids_r.at[spot(d)]))
                counts[d] = counted(spot(d))
                if d == line - 1:

                    @pl.when(head)
                    def _():
                        pl.semaphore_wait(here.at[spot(line - 1)], 1)

            part[c, d] = summed(counts[d], c)
            copy = remote(part.at[c, d], got.at[c, z], part_s.at[c, d], part_r.at[c, z], on_line(d))
            unless(tail, d == line - 1, copy.start)
            part_copies.append((d, copy))
    pl.when(head)(small_line[line - 1].start)
    own = counted(z)
    kept = [summed(own, c) for c in range(CHUNKS)]

    for d in away:
        landed(small.at[spot(d)], sl_r.at[spot(d)])
    small_id, scale_id = column(sid[...], eye), column(cid[...], eye)
    small_rows = jnp.zeros((examples, feats), jnp.float32)
    scale_rows = jnp.zeros((examples, feats), jnp.float32)
    held = small_in.shape[0]
    for b in range(n):
        block = small[b // 2, b % 2].astype(jnp.float32)
        for r in range(held):
            row = block[r : r + 1, :]
            small_rows = jnp.where(small_id == float(b * held + r), row, small_rows)
            scale_rows = jnp.where(scale_id == float(b * held + r), row, scale_rows)
    base = dense[...] * scale_rows

    @pl.when(head)
    def _():
        own_picks = [column(ids[z, p : p + 1, :], eye) for p in range(PICKS)]
        at = [lanes + float((n - 2 + side) * rows) for side in range(2)]
        for c in range(CHUNKS):
            far = jnp.zeros((examples, width), jnp.float32)
            for side in range(2):
                landed(raw.at[side, c], raw_r.at[side, c])
                count = sum(jnp.where(pick == at[side], 1.0, 0.0) for pick in own_picks).astype(jnp.bfloat16)
                far = far + jnp.dot(count, raw[side, c], preferred_element_type=jnp.float32)
            got[c, line - 1] = far

    totals = []
    for c in range(CHUNKS):
        pooled = kept[c]
        for d in range(1, line):
            unless(head, d == line - 1, lambda d=d: landed(got.at[c, spot(d)], part_r.at[c, spot(d)]))
            pooled = pooled + got[c, spot(d)]
        span = slice(c * width, (c + 1) * width)
        totals.append(base[:, span] + pooled * PICKS ** (-0.5) * small_rows[:, span])
    power = sum(jnp.sum(t * t, axis=1, keepdims=True) for t in totals) * (1.0 / feats)
    scale = lax.rsqrt(power + 1e-06)
    for c in range(CHUNKS):
        out[:, cols(c)] = totals[c] * scale
    for copy in tab_copies + [small_pair] + list(small_line.values()):
        copy.wait_send()
    for d, copy in id_copies.items():
        unless(head, d == line - 1, copy.wait_send)
    for d, copy in part_copies:
        unless(tail, d == line - 1, copy.wait_send)

    @pl.when(pusher)
    def _():
        for copy in raw_copies:
            copy.wait_send()


def solution(mesh):
    n = mesh.shape["bank"]
    line = n // 2

    def shards(item_ids, large_table, dense_part, small_ids, small_table, scale_ids):
        rows, feats = large_table.shape
        examples = dense_part.shape[0]
        held = small_table.shape[0]
        width = feats // CHUNKS
        dma = pltpu.SemaphoreType.DMA
        return pl.pallas_call(
            functools.partial(kernel, n),
            out_shape=pltpu.VMEM((examples, feats), jnp.float32),
            in_specs=[pl.BlockSpec(memory_space=pltpu.HBM)] * 6,
            out_specs=pl.BlockSpec(memory_space=pltpu.VMEM),
            scratch_shapes=[
                pltpu.VMEM((line, PICKS, examples), jnp.int32),
                pltpu.VMEM((2, CHUNKS, rows, width), jnp.bfloat16),
                pltpu.VMEM((examples, feats), jnp.float32),
                pltpu.VMEM((1, examples), jnp.int32),
                pltpu.VMEM((line, 2, held, feats), jnp.bfloat16),
                pltpu.VMEM((1, examples), jnp.int32),
                pltpu.VMEM((CHUNKS, line, examples, width), jnp.float32),
                pltpu.VMEM((CHUNKS, line, examples, width), jnp.float32),
                pltpu.VMEM((2, CHUNKS, rows, width), jnp.bfloat16),
                dma((5,)),
                dma((CHUNKS,)),
                dma((line,)),
                dma((line,)),
                dma((CHUNKS,)),
                dma((CHUNKS,)),
                dma((1,)),
                dma((1,)),
                dma((line,)),
                dma((line,)),
                dma((CHUNKS, line)),
                dma((CHUNKS, line)),
                dma((CHUNKS,)),
                dma((2, CHUNKS)),
                pltpu.SemaphoreType.REGULAR,
                pltpu.SemaphoreType.REGULAR((line,)),
            ],
            compiler_params=pltpu.CompilerParams(
                collective_id=0, has_side_effects=True
            ),
        )(
            item_ids.T,
            large_table,
            dense_part,
            small_ids.reshape(1, -1),
            small_table,
            scale_ids.reshape(1, -1),
        )

    return jax.shard_map(
        shards,
        mesh=mesh,
        in_specs=(
            P(("ens", "bank"), None),
            P(("ens", "bank"), None),
            P(("ens", "bank"), None),
            P(("ens", "bank")),
            P(("ens", "bank"), None),
            P(("ens", "bank")),
        ),
        out_specs=P(("ens", "bank"), None),
        check_vma=False,
    )
```
